768 devices in a mesh: grp: 96 (over x, y_lo, z), tbl: 8 (over y_hi, core).
Axes of the slice: x: 4, y: 8 (y_hi: 4, y_lo: 2; y = y_hi * 2 + y_lo), z: 12, core: 2. Of those that a mesh axis runs over, the one named last changes fastest.
Arguments:
- next_ids: int32 [98304, 256], P(('grp', 'tbl')), may hold values from 0 to 6143
- next_lengths: int32 [98304, 26], P(('grp', 'tbl')), may hold values from 1 to 8
- slot_of_table: int32 [26], replicated, may hold values from 0 to 31, as said below
- tables: bfloat16 [32, 6144, 128], P('tbl'), may hold values from -2.5 to 2.5
- cross_input: bfloat16 [98304, 3456], P(('grp', 'tbl')), may hold values from -6 to 6
- cotangent: bfloat16 [98304, 3456], P(('grp', 'tbl')), may hold values from -6 to 6
- up_weight: bfloat16 [256, 3456], replicated, may hold values from -0.375 to 0.375
- down_weight: bfloat16 [3456, 256], replicated, may hold values from -0.109375 to 0.109375
Outputs:
- next_embedded: bfloat16 [98304, 3328], P(('grp', 'tbl'))
- grad_up: float32 [256, 3456], P('tbl', 'grp')
- grad_down: float32 [3456, 256], P('grp', 'tbl')
The draws below stay inside these ranges and needn't reach their ends.
Inputs may be any that keep to these rules, and one draw needn't show every extreme that they name: `next_ids`: entry 8 * s + k of an example's row is the k-th id of the bag held in slot s; entries with k at or past the bag's length, and all entries of slots that hold no table, are padding. `slot_of_table`: distinct slots; owner o along tbl holds slots o * 4 to o * 4 + 3, so an owner holds up to 4 tables and some owner holds exactly 4.
All inputs are finite; a program needn't handle non-finite values.
Results may differ from the reference program's by a relative error of at most 0.0049.
Values may be sent and summed in bfloat16 or wider, within the bound.
A program may use at most 128 MiB of HBM per device.

```python
import math
import jax
import jax.numpy as jnp
import numpy as np
from jax import lax

F = 26
E = 128
R = 256
MAXLEN = 8
ROWS = 6144
B_DEV = 128
D = 3456
TOKENS = 98304
SLOTS_ALL = 32
N_TBL = 8


def draw_slot_of_table(key, part):
    return jax.random.permutation(key, SLOTS_ALL)[:F].astype(jnp.int32)


def plant(entries, stream_key, smallest, top_value):
    shape = entries.shape
    place = [jax.random.randint(jax.random.fold_in(stream_key, axis), (), 0, shape[axis]) for axis in range(len(shape))]
    entries = entries.at[tuple(place)].set(smallest)
    longest = shape.index(max(shape))
    place[longest] = (place[longest] + 1) % shape[longest]
    return entries.at[tuple(place)].set(top_value)


def block_scale(stream_key, shape, split, low, largest):
    loudness, own = 1.0, jax.random.fold_in(stream_key, 6)
    for dim, shards_of in split:
        heights = jnp.exp(jax.random.uniform(jax.random.fold_in(own, dim), (shards_of,), jnp.float32, low / len(split), largest / len(split)))
        loudness = loudness * jnp.repeat(heights, shape[dim] // shards_of).reshape([-1 if axis == dim else 1 for axis in range(len(shape))])
    return loudness


def cumulative_ranks(amount, slope):
    loads = [(1 << 20) // math.isqrt(standing ** slope) + 1 for standing in range(1, amount + 1)]
    deviation = 1 + sum(loads) // (1 << 30)
    return np.cumsum(np.array([max(1, weight // deviation) for weight in loads]))


def ranked_ids(key, extent, number_of, lean):
    table = cumulative_ranks(number_of, lean)
    pick = jax.random.randint(jax.random.fold_in(key, 1), extent, 0, int(table[number_of - 1]))
    grade = jnp.searchsorted(jnp.asarray(table, jnp.int32), pick, side="right")
    return jax.random.permutation(jax.random.fold_in(key, 2), number_of)[grade].astype(jnp.int32)


def gaussian(rng, extent, width, most, cuts=(), kind=jnp.bfloat16):
    entries = jax.random.normal(rng, extent, jnp.float32) * width
    if len(cuts) > 0:
        entries = block_scale(rng, extent, cuts, -0.22, 0.18) * entries
    return jnp.clip(entries, min=-most, max=most).astype(kind)


def setup_inputs(seed: int = 0) -> dict:
    key_list = jax.random.split(jax.random.key(seed), 9)
    return {
        "next_ids": plant(ranked_ids(key_list[0], (TOKENS, SLOTS_ALL * MAXLEN), ROWS, 2), jax.random.fold_in(key_list[0], 3), 0, ROWS - 1).astype(jnp.int32),
        "next_lengths": plant(jax.random.randint(key_list[1], (TOKENS, F), 1, MAXLEN + 1), jax.random.fold_in(key_list[1], 1), 1, MAXLEN).astype(jnp.int32),
        "slot_of_table": draw_slot_of_table(jax.random.fold_in(key_list[8], 71), 0),
        "tables": gaussian(key_list[3], (SLOTS_ALL, ROWS, E), 0.35, 2.5, ((0, 8),)),
        "cross_input": gaussian(key_list[4], (TOKENS, D), 1.0, 6.0, ((0, 768),)),
        "cotangent": gaussian(key_list[5], (TOKENS, D), 1.0, 6.0, ((0, 768),)),
        "up_weight": gaussian(key_list[6], (R, D), R ** -0.5, 0.375),
        "down_weight": gaussian(key_list[7], (D, R), D ** -0.5, 0.109375),
    }


def pool_block(tables, slot_of_table, ids, lengths):
    count = ids.shape[0]
    ids_three = ids.reshape(count, SLOTS_ALL, MAXLEN)
    chosen = jnp.take(ids_three, slot_of_table, axis=1)
    flat_table = tables.reshape(SLOTS_ALL * ROWS, E)
    index = (chosen + (slot_of_table * ROWS)[None, :, None]).astype(jnp.int32)
    picked = jnp.take(flat_table, index.reshape(-1), axis=0).reshape(count, F, MAXLEN, E)
    keep = lax.broadcasted_iota(jnp.int32, (count, F, MAXLEN), 2) < lengths[:, :, None]
    masked = jnp.where(keep[..., None], picked, jnp.zeros((), picked.dtype))
    pooled = lax.optimization_barrier(jnp.sum(masked.astype(jnp.float32), axis=2))
    return pooled.astype(jnp.bfloat16).reshape(count, F * E)

def reference(next_ids, next_lengths, slot_of_table, tables, cross_input, cotangent, up_weight, down_weight):
    blocks = TOKENS // B_DEV
    id_blocks = next_ids.reshape(blocks, B_DEV, SLOTS_ALL * MAXLEN)
    len_blocks = next_lengths.reshape(blocks, B_DEV, F)
    pooled = lax.map(lambda pair: pool_block(tables, slot_of_table, pair[0], pair[1]), (id_blocks, len_blocks))
    next_embedded = pooled.reshape(TOKENS, F * E)
    span = B_DEV * N_TBL
    input_blocks = cross_input.reshape(TOKENS // span, span, D)
    grad_blocks = cotangent.reshape(TOKENS // span, span, D)

    def step(carry, pair):
        total_up, total_down = carry
        inputs, grads = pair
        low = jnp.dot(inputs, down_weight, preferred_element_type=jnp.float32).astype(jnp.bfloat16)
        dz = (grads.astype(jnp.float32) * inputs.astype(jnp.float32)).astype(jnp.bfloat16)
        dlow = jnp.dot(dz, up_weight.T, preferred_element_type=jnp.float32).astype(jnp.bfloat16)
        total_up = total_up + jnp.dot(low.T, dz, preferred_element_type=jnp.float32)
        total_down = total_down + jnp.dot(inputs.T, dlow, preferred_element_type=jnp.float32)
        return ((total_up, total_down), None)
    start = (jnp.zeros((R, D), jnp.float32), jnp.zeros((D, R), jnp.float32))
    (total_up, total_down), unused = lax.scan(step, start, (input_blocks, grad_blocks))
    factor = 1.0 / math.sqrt(TOKENS)
    return (next_embedded, total_up * factor, total_down * factor)
```

```python
import functools
import math

import jax
import jax.numpy as jnp
from jax import lax
from jax.experimental import pallas as pl
from jax.experimental.pallas import tpu as pltpu
from jax.sharding import PartitionSpec as P

MESH = pl.DeviceIdType.MESH
F32 = jnp.float32
BF16 = jnp.bfloat16

X, YH, YL, Z = 4, 4, 2, 12
Y = YH * YL
UNROLL = 16
REACH = (0, 2, -1, -3)
SERVE = (6, 7, 2, 3, 4, 5, 1, 0)
FAR = (6, 5, 7, 4, 8, 3, 9, 2, 10, 1, 11)


def kernel(
    ids_hbm,
    lens_ref,
    slot_row_ref,
    slot_ref,
    tables_hbm,
    x_hbm,
    c_hbm,
    up_hbm,
    down_hbm,
    emb_ref,
    gup_ref,
    gdown_ref,
    ids_v,
    words,
    got_words,
    words_s,
    tab_b,
    tab,
    x_v,
    c_v,
    up_v,
    down_v,
    dz_v,
    low_v,
    dlow_v,
    half_out,
    half_in,
    own,
    xs,
    x_relay_in,
    x_direct,
    x_relay_out,
    x_summed,
    sx,
    zs,
    zr,
    ys,
    yr,
    turned,
    bags,
    pooled,
    arrived,
    ld_sem,
    ids_s,
    ids_r,
    pair_s,
    pair_r,
    xa_s,
    xa_r,
    xb_s,
    xb_r,
    xc_s,
    xc_r,
    z_s,
    z_r,
    y_s,
    y_r,
    e_s,
    e_r,
):
    g = lax.axis_index("grp")
    t = lax.axis_index("tbl")
    x, yl, z = g // (YL * Z), (g // Z) % YL, g % Z
    yh, c = t // 2, t % 2
    y = yh * 2 + yl
    sign = 1 - 2 * yl
    rows_flat = tables_hbm.shape[0]
    rows_each = rows_flat // 4
    width = x_hbm.shape[1]
    per_x = width // X
    per_y = per_x // YL
    per_z = per_y // Z
    examples = ids_hbm.shape[0]

    def place(px, py, pz, pc):
        return ((px * YL + py % 2) * Z + pz, (py // 2) * 2 + pc)

    def remote(src, dst, send, recv, where):
        return pltpu.make_async_remote_copy(
            src_ref=src, dst_ref=dst, send_sem=send, recv_sem=recv, device_id=where, device_id_type=MESH
        )

    loads = [
        pltpu.make_async_copy(src, dst, ld_sem.at[i])
        for i, (src, dst) in enumerate(
            (
                (ids_hbm, ids_v),
                (x_hbm, x_v),
                (down_hbm, down_v),
                (c_hbm, c_v),
                (up_hbm, up_v),
                (tables_hbm, tab_b),
            )
        )
    ]
    for load in loads:
        load.start()

    barrier = pltpu.get_barrier_semaphore()
    met = 0
    for dy in range(Y):
        for b in range(2):
            if dy or b:
                pl.semaphore_signal(
                    barrier, inc=1, device_id=place(x, (y + dy) % Y, z, (c + b) % 2), device_id_type=MESH
                )
                met += 1
    for dx in (1, X - 1):
        pl.semaphore_signal(barrier, inc=1, device_id=place((x + dx) % X, y, z, c), device_id_type=MESH)
        met += 1
    for dz in range(1, Z):
        pl.semaphore_signal(barrier, inc=1, device_id=place(x, y, (z + dz) % Z, c), device_id_type=MESH)
        met += 1

    loads[0].wait()
    entries = ids_hbm.shape[1]
    spread = (lax.broadcasted_iota(jnp.int32, (entries, slot_row_ref.shape[1]), 0) // 8 == slot_row_ref[...]).astype(BF16)
    lens = lax.dot_general(
        spread, lens_ref[...].astype(F32).astype(BF16), (((1,), (1,)), ((), ())), preferred_element_type=F32
    )
    entry = lax.broadcasted_iota(jnp.int32, (entries, examples), 0)
    local = jnp.transpose(ids_v[...]) + ((entry // 8) % 4) * rows_each
    local = jnp.where((entry % 8).astype(F32) < lens, local, rows_flat)
    by_owner = local.reshape(8, 2, 16, examples)
    words[...] = by_owner[:, 0] + by_owner[:, 1] * 65536

    pl.semaphore_wait(barrier, met)

    ids_copies = {}
    for r in range(1, 8):
        py, pc = (y + sign * REACH[r // 2] + Y) % Y, (c + r % 2) % 2
        ids_copies[r] = remote(
            words.at[(py // 2) * 2 + pc], got_words.at[r], ids_s.at[r], ids_r.at[r], place(x, py, z, pc)
        )
        ids_copies[r].start()
    to_smem = [
        pltpu.make_async_copy(words.at[t] if r == 0 else got_words.at[r], words_s.at[r], ld_sem.at[6 + r])
        for r in range(8)
    ]
    to_smem[0].start()

    loads[1].wait()
    loads[2].wait()
    col = lax.broadcasted_iota(jnp.int32, (256, 256), 1)
    row = lax.broadcasted_iota(jnp.int32, (256, 256), 0)
    core = jnp.where(col < 128, 1 - c, c)
    order = (row == (((col % 128) // 32) * 2 + core) * 32 + col % 32).astype(BF16)
    low = jnp.dot(x_v[...], down_v[...], preferred_element_type=F32).astype(BF16)
    low_v[...] = jnp.dot(low, order, preferred_element_type=F32).astype(BF16)
    loads[3].wait()
    loads[4].wait()
    dz_v[...] = (c_v[...].astype(F32) * x_v[...].astype(F32)).astype(BF16)
    dlow = lax.dot_general(
        dz_v[...], up_v[...], (((1,), (1,)), ((), ())), preferred_element_type=F32
    ).astype(BF16)
    dlow_v[...] = jnp.dot(dlow, order, preferred_element_type=F32).astype(BF16)

    def partials(i, carry):
        r0 = pl.multiple_of(i * 384, 128)
        for k, (left, right) in enumerate(((dz_v, low_v), (x_v, dlow_v))):
            part = lax.dot_general(
                left[:, pl.ds(r0, 384)], right[...], (((0,), (0,)), ((), ())), preferred_element_type=F32
            )
            half_out[k, pl.ds(r0, 384), :] = part[:, :128].astype(BF16)
            own[k, pl.ds(r0, 384), :] = part[:, 128:]
        return carry

    lax.fori_loop(0, width // 384, partials, 0)

    block = [((x + d) % X) * per_x for d in (2, 1, X - 1, 0)]
    pair = []
    for j in range(4):
        rows = pl.ds(pl.multiple_of(block[j], 16), per_x)
        pair.append(
            remote(
                half_out.at[:, rows], half_in.at[:, rows], pair_s.at[j], pair_r.at[j], place(x, y, z, (c + 1) % 2)
            )
        )
        pair[j].start()

    loads[5].wait()

    def widen(i, carry):
        r0 = pl.multiple_of(i * 256, 256)
        tab[pl.ds(r0, 256), :] = tab_b[pl.ds(r0, 256), :].astype(F32)
        return carry

    lax.fori_loop(0, rows_flat // 256, widen, 0)
    tab[pl.ds(rows_flat, 8), :] = jnp.zeros((8, 128), F32)

    step = 144

    def chip_sum(k, start):
        rows = pl.ds(pl.multiple_of(start, 16), step)
        return own[k, rows, :] + half_in[k, rows, :].astype(F32)

    def stage(j, kinds):
        def body(i, carry):
            for k in kinds:
                start = block[j] + i * step
                xs[k, pl.ds(pl.multiple_of(start, 16), step), :] = chip_sum(k, start).astype(BF16)
            return carry

        lax.fori_loop(0, per_x // step, body, 0)

    ahead, behind = place((x + 1) % X, y, z, c), place((x + X - 1) % X, y, z, c)

    def x_rows(j):
        return pl.ds(pl.multiple_of(block[j], 16), per_x)

    pair[0].wait_recv()
    stage(0, (0, 1))
    relay = [
        remote(xs.at[0, x_rows(0)], x_relay_in.at[0], xa_s.at[0], xa_r.at[0], ahead),
        remote(xs.at[1, x_rows(0)], x_relay_in.at[1], xa_s.at[1], xa_r.at[1], behind),
    ]
    for copy in relay:
        copy.start()
    pair[1].wait_recv()
    stage(1, (1,))
    pair[2].wait_recv()
    stage(2, (0,))
    direct = [
        remote(xs.at[1, x_rows(1)], x_direct.at[1], xb_s.at[0], xb_r.at[0], ahead),
        remote(xs.at[0, x_rows(2)], x_direct.at[0], xb_s.at[1], xb_r.at[1], behind),
    ]
    for copy in direct:
        copy.start()

    for r in range(1, 8):
        ids_copies[r].wait_recv()
        to_smem[r].start()
    for r in range(8):
        to_smem[r].wait()

    def pool(r):
        def body(i, carry):
            a = i // (examples // UNROLL)
            e = (i % (examples // UNROLL)) * UNROLL
            for u in range(UNROLL):
                low_rows, high_rows = [], []
                for k in range(8):
                    word = words_s[r, a * 8 + k, e + u]
                    low_rows.append(tab[pl.ds(word & 0xFFFF, 1), :])
                    high_rows.append(tab[pl.ds(lax.shift_right_logical(word, 16), 1), :])
                for half, picked in enumerate((low_rows, high_rows)):
                    while len(picked) > 1:
                        picked = [picked[n] + picked[n + 1] for n in range(0, len(picked), 2)]
                    bags[half, pl.ds(u, 1), :] = picked[0]
            at = pl.ds(pl.multiple_of(e, UNROLL), UNROLL)
            for half in range(2):
                if r == 0:
                    arrived[t * 4 + a + 2 * half, at, :] = bags[half].astype(BF16)
                else:
                    pooled[r, a + 2 * half, at, :] = bags[half].astype(BF16)
            return carry

        lax.fori_loop(0, 2 * (examples // UNROLL), body, 0)
        if r == 0:
            return None
        py, pc = (y + (-sign if r // 2 == 1 else sign) * (REACH[r // 2]) + 2 * Y) % Y, (c + r % 2) % 2
        copy = remote(
            pooled.at[r], arrived.at[pl.ds(t * 4, 4)], e_s.at[r], e_r.at[r], place(x, py, z, pc)
        )
        copy.start()
        return copy

    sent = [pool(SERVE[0])]

    for copy in relay:
        copy.wait_recv()

    def add_relay(i, carry):
        rows = pl.ds(pl.multiple_of(i * step, 16), step)
        for k in range(2):
            total = chip_sum(k, block[1 + k] + i * step) + x_relay_in[k, rows, :].astype(F32)
            x_relay_out[k, rows, :] = total.astype(BF16)
        return carry

    lax.fori_loop(0, per_x // step, add_relay, 0)
    summed = [
        remote(x_relay_out.at[0], x_summed.at[0], xc_s.at[0], xc_r.at[0], ahead),
        remote(x_relay_out.at[1], x_summed.at[1], xc_s.at[1], xc_r.at[1], behind),
    ]
    for copy in summed:
        copy.start()

    for n in (1, 2):
        sent.append(pool(SERVE[n]))

    pair[3].wait_recv()
    for copy in direct:
        copy.wait_recv()
    for copy in summed:
        copy.wait_recv()

    def add_x(i, carry):
        rows = pl.ds(pl.multiple_of(i * step, 16), step)
        for k in range(2):
            total = chip_sum(k, block[3] + i * step)
            sx[k, rows, :] = total + x_direct[k, rows, :].astype(F32) + x_summed[k, rows, :].astype(F32)
        return carry

    lax.fori_loop(0, per_x // step, add_x, 0)
    spare = jnp.zeros((8, 128), F32)
    for pz in range(Z):
        for k in range(2):
            parts = [sx[k, n * per_y + pz * per_z : n * per_y + (pz + 1) * per_z, :] for n in range(YL)]
            zs[pz, k, :, :] = jnp.concatenate(parts + [spare], axis=0).astype(BF16)
    along_z = []
    for d in FAR:
        pz = (z + d) % Z
        along_z.append(remote(zs.at[pz], zr.at[d - 1], z_s.at[d], z_r.at[d], place(x, y, pz, c)))
        along_z[-1].start()

    for n in (3, 4, 5, 6):
        sent.append(pool(SERVE[n]))

    for copy in along_z:
        copy.wait_recv()
    both = [zs[z, k, :, :].astype(F32) for k in range(2)]
    for d in range(1, Z):
        both = [both[k] + zr[d - 1, k, :, :].astype(F32) for k in range(2)]
    for n in range(YL):
        rows = slice(n * per_z, (n + 1) * per_z)
        ys[n, :, :] = jnp.concatenate([both[0][rows], both[1][rows], spare], axis=0).astype(BF16)
    along_y = []
    for d in (4, 3, 5, 2, 6, 1, 7):
        py = (y + d) % Y
        along_y.append(remote(ys.at[py % 2], yr.at[d - 1], y_s.at[d], y_r.at[d], place(x, py, z, c)))
        along_y[-1].start()

    pool(SERVE[7])

    for copy in along_y:
        copy.wait_recv()
    total = ys[yl, :, :].astype(F32)
    for d in range(1, Y):
        total = total + yr[d - 1, :, :].astype(F32)
    total = total * (1.0 / math.sqrt(examples * X * Y * Z * 2))
    turned[...] = jnp.transpose(jnp.concatenate([total, jnp.zeros((128 - total.shape[0], 128), F32)], axis=0))
    gup_ref[...] = turned[pl.ds(pl.multiple_of(yh * 32, 32), 32), 0:per_z]
    mine = jnp.zeros((per_z, 32), F32)
    for n in range(YH):
        mine = jnp.where(yh == n, total[per_z : 2 * per_z, n * 32 : (n + 1) * 32], mine)
    gdown_ref[...] = mine

    for copy in sent:
        copy.wait_recv()
    for f in range(slot_ref.shape[0]):
        emb_ref[:, f * 128 : (f + 1) * 128] = arrived[slot_ref[f], :, :]

    for copy in [*ids_copies.values(), *pair, *relay, *direct, *summed, *along_z, *along_y, *sent]:
        copy.wait_send()


def on_device(
    next_ids, next_lengths, slot_of_table, tables, cross_input, cotangent, up_weight, down_weight
):
    examples, entries = next_ids.shape
    feats = slot_of_table.shape[0]
    slots, rows_each, embed = tables.shape
    width = cross_input.shape[1]
    rank = up_weight.shape[0]
    per_x = width // X
    per_z = per_x // YL // Z
    whole = pl.BlockSpec(memory_space=pltpu.VMEM)
    anywhere = pl.BlockSpec(memory_space=pl.ANY)
    vmem, dma = pltpu.VMEM, pltpu.SemaphoreType.DMA
    return pl.pallas_call(
        kernel,
        out_shape=(
            jax.ShapeDtypeStruct((examples, feats * embed), BF16),
            jax.ShapeDtypeStruct((32, per_z), F32),
            jax.ShapeDtypeStruct((per_z, 32), F32),
        ),
        in_specs=[
            anywhere,
            whole,
            whole,
            pl.BlockSpec(memory_space=pltpu.SMEM),
            anywhere,
            anywhere,
            anywhere,
            anywhere,
            anywhere,
        ],
        out_specs=(whole, whole, whole),
        scratch_shapes=[
            vmem((examples, entries), jnp.int32),
            vmem((8, 16, examples), jnp.int32),
            vmem((8, 16, examples), jnp.int32),
            pltpu.SMEM((8, 16, examples), jnp.int32),
            vmem((slots * rows_each, embed), BF16),
            vmem((slots * rows_each + 8, embed), F32),
            vmem((examples, width), BF16),
            vmem((examples, width), BF16),
            vmem((rank, width), BF16),
            vmem((width, rank), BF16),
            vmem((examples, width), BF16),
            vmem((examples, rank), BF16),
            vmem((examples, rank), BF16),
            vmem((2, width, 128), BF16),
            vmem((2, width, 128), BF16),
            vmem((2, width, 128), F32),
            vmem((2, width, 128), BF16),
            vmem((2, per_x, 128), BF16),
            vmem((2, per_x, 128), BF16),
            vmem((2, per_x, 128), BF16),
            vmem((2, per_x, 128), BF16),
            vmem((2, per_x, 128), F32),
            vmem((Z, 2, 80, 128), BF16),
            vmem((Z - 1, 2, 80, 128), BF16),
            vmem((YL, 80, 128), BF16),
            vmem((Y - 1, 80, 128), BF16),
            vmem((128, 128), F32),
            vmem((2, UNROLL, embed), F32),
            vmem((8, 4, examples, embed), BF16),
            vmem((32, examples, embed), BF16),
            dma((14,)),
            dma((8,)),
            dma((8,)),
            dma((4,)),
            dma((4,)),
            dma((2,)),
            dma((2,)),
            dma((2,)),
            dma((2,)),
            dma((2,)),
            dma((2,)),
            dma((Z,)),
            dma((Z,)),
            dma((Y,)),
            dma((Y,)),
            dma((8,)),
            dma((8,)),
        ],
        compiler_params=pltpu.CompilerParams(
            collective_id=0, has_side_effects=True, vmem_limit_bytes=60 * 2**20
        ),
    )(
        next_ids,
        next_lengths,
        slot_of_table.reshape(1, feats),
        slot_of_table,
        tables.reshape(slots * rows_each, embed),
        cross_input,
        cotangent,
        up_weight,
        down_weight,
    )


def solution(mesh):
    return jax.shard_map(
        on_device,
        mesh=mesh,
        in_specs=(
            P(("grp", "tbl"), None),
            P(("grp", "tbl"), None),
            P(),
            P("tbl", None, None),
            P(("grp", "tbl"), None),
            P(("grp", "tbl"), None),
            P(),
            P(),
        ),
        out_specs=(P(("grp", "tbl"), None), P("tbl", "grp"), P("grp", "tbl")),
        check_vma=False,
    )
```

```python
import math

import jax
import jax.numpy as jnp
from jax import lax
from jax.experimental import pallas as pl
from jax.experimental.pallas import tpu as pltpu
from jax.sharding import PartitionSpec as P

MESH = pl.DeviceIdType.MESH
F32 = jnp.float32
BF16 = jnp.bfloat16

X, YH, YL, Z = 4, 4, 2, 12
Y = YH * YL
REACH = (0, -1, 2, -3)
FAR = (6, 5, 7, 4, 8, 3, 9, 2, 10, 1, 11)


def kernel(
    ids_hbm,
    lens_hbm,
    slot_row_hbm,
    tables_hbm,
    x_hbm,
    c_hbm,
    up_hbm,
    down_hbm,
    arrived,
    gup_hbm,
    gdown_hbm,
    ids_v,
    lens_v,
    slot_row_v,
    words,
    got_words,
    local_ids,
    window,
    tab_b,
    tab,
    x_v,
    c_v,
    up_v,
    down_v,
    dz_v,
    low_v,
    dlow_v,
    half_out,
    half_in,
    own,
    xs,
    x_relay_in,
    x_direct,
    x_relay_out,
    x_summed,
    sx,
    zs,
    zr,
    ys,
    yr,
    turned,
    gup_v,
    gdown_v,
    bags,
    pooled,
    ld_sem,
    win_sem,
    ids_s,
    ids_r,
    pair_s,
    pair_r,
    xa_s,
    xa_r,
    xb_s,
    xb_r,
    xc_s,
    xc_r,
    z_s,
    z_r,
    y_s,
    y_r,
    e_s,
    e_r,
):
    g = lax.axis_index("grp")
    t = lax.axis_index("tbl")
    x, yl, z = g // (YL * Z), (g // Z) % YL, g % Z
    yh, c = t // 2, t % 2
    y = yh * 2 + yl
    sign = 1 - 2 * yl
    rows_flat = tables_hbm.shape[0]
    rows_each = rows_flat // 4
    width = x_hbm.shape[1]
    per_x = width // X
    per_y = per_x // YL
    per_z = per_y // Z
    examples, entries = ids_hbm.shape

    def place(px, py, pz, pc):
        return ((px * YL + py % 2) * Z + pz, (py // 2) * 2 + pc)

    def remote(src, dst, send, recv, where):
        return pltpu.make_async_remote_copy(
            src_ref=src, dst_ref=dst, send_sem=send, recv_sem=recv, device_id=where, device_id_type=MESH
        )

    loads = [
        pltpu.make_async_copy(src, dst, ld_sem.at[i])
        for i, (src, dst) in enumerate(
            (
                (lens_hbm, lens_v),
                (slot_row_hbm, slot_row_v),
                (ids_hbm, ids_v),
                (x_hbm, x_v),
                (down_hbm, down_v),
                (c_hbm, c_v),
                (up_hbm, up_v),
                (tables_hbm, tab_b),
            )
        )
    ]
    for load in loads:
        load.start()

    barrier = pltpu.get_barrier_semaphore()
    met = 0
    for dy in range(Y):
        for b in range(2):
            if dy or b:
                pl.semaphore_signal(
                    barrier, inc=1, device_id=place(x, (y + dy) % Y, z, (c + b) % 2), device_id_type=MESH
                )
                met += 1
    for dx in (1, X - 1):
        pl.semaphore_signal(barrier, inc=1, device_id=place((x + dx) % X, y, z, c), device_id_type=MESH)
        met += 1
    for dz in range(1, Z):
        pl.semaphore_signal(barrier, inc=1, device_id=place(x, y, (z + dz) % Z, c), device_id_type=MESH)
        met += 1

    loads[3].wait()
    loads[4].wait()
    col = lax.broadcasted_iota(jnp.int32, (256, 256), 1)
    row = lax.broadcasted_iota(jnp.int32, (256, 256), 0)
    core = jnp.where(col < 128, 1 - c, c)
    order = (row == (((col % 128) // 32) * 2 + core) * 32 + col % 32).astype(BF16)
    low = jnp.dot(x_v[...], down_v[...], preferred_element_type=F32).astype(BF16)
    low_v[...] = jnp.dot(low, order, preferred_element_type=F32).astype(BF16)
    loads[5].wait()
    loads[6].wait()
    dz_v[...] = (c_v[...].astype(F32) * x_v[...].astype(F32)).astype(BF16)
    dlow = lax.dot_general(
        dz_v[...], up_v[...], (((1,), (1,)), ((), ())), preferred_element_type=F32
    ).astype(BF16)
    dlow_v[...] = jnp.dot(dlow, order, preferred_element_type=F32).astype(BF16)

    pl.semaphore_wait(barrier, met)
    for n in range(3):
        loads[n].wait()
    spread = (lax.broadcasted_iota(jnp.int32, (entries, slot_row_v.shape[1]), 0) // 8 == slot_row_v[...]).astype(BF16)
    lens = lax.dot_general(
        spread, lens_v[...].astype(F32).astype(BF16), (((1,), (0,)), ((), ())), preferred_element_type=F32
    )
    entry = lax.broadcasted_iota(jnp.int32, (entries, examples), 0)
    local = jnp.transpose(ids_v[...]) + ((entry // 8) % 4) * rows_each
    local = jnp.where((entry % 8).astype(F32) < lens, local, rows_flat)
    by_owner = local.reshape(8, 2, 16, examples)
    words[...] = by_owner[:, 0] + by_owner[:, 1] * 65536

    def ids_copy(r):
        py, pc = (y + sign * REACH[r // 2] + Y) % Y, (c + r % 2) % 2
        return remote(words.at[(py // 2) * 2 + pc], got_words.at[r], ids_s.at[r], ids_r.at[r], place(x, py, z, pc))

    for r in range(7, 0, -1):
        ids_copy(r).start()

    step = 144

    def chip_sum(k, start):
        rows = pl.ds(pl.multiple_of(start, 16), step)
        return own[k, rows, :] + half_in[k, rows, :].astype(F32)

    def stage(j, q, k):
        def body(i, carry):
            start = first_row(j, q) + i * step
            xs[k, pl.ds(pl.multiple_of(start, 16), step), :] = chip_sum(k, start).astype(BF16)
            return carry

        lax.fori_loop(0, per_y // step, body, 0)

    ahead, behind = place((x + 1) % X, y, z, c), place((x + X - 1) % X, y, z, c)

    def relay(q, k):
        n = 2 * q + k
        where = (ahead, behind)[k]
        return remote(xs.at[k, rows_of(0, q)], x_relay_in.at[q, k], xa_s.at[n], xa_r.at[n], where)

    def direct(q, k):
        n = 2 * q + k
        where = (behind, ahead)[k]
        return remote(xs.at[k, rows_of(2 - k, q)], x_direct.at[q, k], xb_s.at[n], xb_r.at[n], where)

    def summed(q, k):
        n = 2 * q + k
        where = (ahead, behind)[k]
        return remote(x_relay_out.at[q, k], x_summed.at[q, k], xc_s.at[n], xc_r.at[n], where)

    def along_z(q, d):
        pz, n = (z + d) % Z, q * Z + d
        return remote(zs.at[q, pz], zr.at[q, d - 1], z_s.at[n], z_r.at[n], place(x, y, pz, c))

    def along_y(d):
        return remote(ys.at[d % 2], yr.at[d - 1], y_s.at[d], y_r.at[d], place(x, (y + d) % Y, z, c))

    def x_relay(q):
        pair(0, q).wait_recv()
        for k in range(2):
            stage(0, q, k)
            relay(q, k).start()

    def x_near(q):
        for k in range(2):
            pair(2 - k, q).wait_recv()
            stage(2 - k, q, k)
            direct(q, k).start()

    def x_forward(q):
        for k in range(2):
            relay(q, k).wait_recv()

            def body(i, carry, k=k):
                rows = pl.ds(pl.multiple_of(i * step, 16), step)
                total = chip_sum(k, first_row(1 + k, q) + i * step) + x_relay_in[q, k, rows, :].astype(F32)
                x_relay_out[q, k, rows, :] = total.astype(BF16)
                return carry

            lax.fori_loop(0, per_y // step, body, 0)
            summed(q, k).start()

    def z_send(q):
        pair(3, q).wait_recv()
        for k in range(2):
            direct(q, k).wait_recv()
            summed(q, k).wait_recv()

        def body(i, carry):
            rows = pl.ds(pl.multiple_of(i * step, 16), step)
            for k in range(2):
                total = chip_sum(k, first_row(3, q) + i * step)
                total = total + x_direct[q, k, rows, :].astype(F32) + x_summed[q, k, rows, :].astype(F32)
                sx[k, rows, :] = total
            return carry

        lax.fori_loop(0, per_y // step, body, 0)
        spare = jnp.zeros((8, 128), F32)
        for pz in range(Z):
            parts = [sx[k, pz * per_z : (pz + 1) * per_z, :] for k in range(2)]
            zs[q, pz, :, :] = jnp.concatenate(parts + [spare], axis=0).astype(BF16)
        for d in FAR:
            along_z(q, d).start()

    def y_send(q):
        total = zs[q, z, :, :].astype(F32)
        for d in FAR:
            along_z(q, d).wait_recv()
            total = total + zr[q, d - 1, :, :].astype(F32)
        ys[q, :, :] = total.astype(BF16)
        for d in ((4, 2, 6), (3, 5, 1, 7))[q]:
            along_y(d).start()

    tiles = width // 384
    first_tile = ((x + 2) % X) * per_x // 384

    def partials(i, carry):
        r0 = pl.multiple_of(((i + first_tile) % tiles) * 384, 128)
        for k, (left, right) in enumerate(((dz_v, low_v), (x_v, dlow_v))):
            part = lax.dot_general(
                left[:, pl.ds(r0, 384)], right[...], (((0,), (0,)), ((), ())), preferred_element_type=F32
            )
            half_out[k, pl.ds(r0, 384), :] = part[:, :128].astype(BF16)
            own[k, pl.ds(r0, 384), :] = part[:, 128:]
        return carry

    part_of = [yl, 1 - yl]

    def first_row(j, q):
        return ((x + (2, 1, X - 1, 0)[j]) % X) * per_x + part_of[q] * per_y

    def rows_of(j, q):
        return pl.ds(pl.multiple_of(first_row(j, q), 16), per_y)

    def pair(j, q):
        rows, n = rows_of(j, q), 2 * j + q
        return remote(
            half_out.at[:, rows], half_in.at[:, rows], pair_s.at[n], pair_r.at[n], place(x, y, z, (c + 1) % 2)
        )

    lax.fori_loop(0, tiles // 3, partials, 0)
    pair(0, 0).start()
    lax.fori_loop(tiles // 3, 2 * tiles // 3, partials, 0)
    pair(2, 0).start()
    lax.fori_loop(2 * tiles // 3, tiles, partials, 0)
    for j, q in ((1, 0), (0, 1), (1, 1), (2, 1), (3, 0), (3, 1)):
        pair(j, q).start()

    x_relay(0)
    loads[7].wait()

    def widen(i, carry):
        r0 = pl.multiple_of(i * 256, 256)
        tab[pl.ds(r0, 256), :] = tab_b[pl.ds(r0, 256), :].astype(F32)
        return carry

    lax.fori_loop(0, rows_flat // 256, widen, 0)
    tab[pl.ds(rows_flat, 8), :] = jnp.zeros((8, 128), F32)

    x_near(0)

    local_words = [words[t]]
    for r in range(1, 8):
        ids_copy(r).wait_recv()
        local_words.append(got_words[r])
    for r in range(8):
        pair_of = local_words[r].reshape(2, 8, examples)
        local_ids[r, 0:2] = pair_of & 0xFFFF
        local_ids[r, 2:4] = lax.shift_right_logical(pair_of, 16)

    def refill(r, slot, s):
        return pltpu.make_async_copy(local_ids.at[r, slot], window.at[s], win_sem.at[s])

    def partner(n):
        far, other = 3 - n // 2, (n + n // 6) % 2
        return 2 * far + other, far, other

    def bags_to(n):
        r, far, other = partner(n)
        where = place(x, (y - sign * far + Y) % Y, z, (c + other) % 2)
        return remote(pooled.at[r], arrived.at[pl.ds(t * 4, 4)], e_s.at[r], e_r.at[r], where)

    for s in range(2):
        refill(partner(0)[0], s, s).start()

    events = {2: [(x_forward, 0), (x_relay, 1), (x_near, 1)], 6: [(z_send, 0)], 8: [(x_forward, 1)], 12: [(z_send, 1)]}

    def pool(i, carry):
        for at, steps in events.items():

            @pl.when(i == at)
            def _(steps=steps):
                for act, q in steps:
                    act(q)

        n, j = i // 2, i % 2
        r, after = partner(n)[0], partner(n + 1)[0]
        for s in range(2):
            slot = 2 * j + s
            refill(r, slot, s).wait()
            for u in range(examples):
                picked = [tab[pl.ds(window[s, k, u], 1), :] for k in range(8)]
                while len(picked) > 1:
                    picked = [picked[m] + picked[m + 1] for m in range(0, len(picked), 2)]
                bags[s * examples + u : s * examples + u + 1, :] = picked[0]

            @pl.when(i < 15)
            def _(s=s):
                refill(r * (1 - j) + after * j, (2 + s) * (1 - j) + s * j, s).start()

        for s in range(2):
            pooled[r, 2 * j + s, :, :] = bags[s * examples : (s + 1) * examples, :].astype(BF16)

        @pl.when((j == 1) & (n < 7))
        def _():
            bags_to(n).start()

        return carry

    lax.fori_loop(0, 16, pool, 0)
    sent = [bags_to(n) for n in range(7)]
    sent.append(pltpu.make_async_copy(pooled.at[0], arrived.at[pl.ds(t * 4, 4)], e_s.at[0]))
    sent[7].start()
    y_send(0)
    y_send(1)
    total = ys[0, :, :].astype(F32)
    for d in (4, 2, 6, 3, 5, 1, 7):
        along_y(d).wait_recv()
        total = total + yr[d - 1, :, :].astype(F32)
    total = total * (1.0 / math.sqrt(examples * X * Y * Z * 2))
    turned[...] = jnp.transpose(jnp.concatenate([total, jnp.zeros((128 - total.shape[0], 128), F32)], axis=0))
    gup_v[...] = turned[pl.ds(pl.multiple_of(yh * 32, 32), 32), 0:per_z]
    gdown_v[...] = turned[pl.ds(pl.multiple_of(yh * 32, 32), 32), per_z : 2 * per_z]
    outs = [
        pltpu.make_async_copy(gup_v, gup_hbm, ld_sem.at[0]),
        pltpu.make_async_copy(gdown_v, gdown_hbm, ld_sem.at[1]),
    ]
    for out in outs:
        out.start()

    for copy in sent[:7]:
        copy.wait_recv()
        copy.wait_send()
    for r in range(1, 8):
        ids_copy(r).wait_send()
    for q in range(2):
        for j in range(4):
            pair(j, q).wait_send()
        for k in range(2):
            for copy in (relay, direct, summed):
                copy(q, k).wait_send()
        for d in FAR:
            along_z(q, d).wait_send()
    for d in range(1, Y):
        along_y(d).wait_send()
    sent[7].wait()
    for out in outs:
        out.wait()


def finish(slot_ref, arrived_hbm, gup_in, gdown_in, emb_hbm, gup_hbm, gdown_hbm, emb_v, gup_v, gdown_v, sem):
    feats = slot_ref.shape[0]
    small = [
        (pltpu.make_async_copy(src, mid, sem.at[n]), pltpu.make_async_copy(mid, dst, sem.at[n]))
        for n, (src, mid, dst) in enumerate(((gup_in, gup_v, gup_hbm), (gdown_in, gdown_v, gdown_hbm)))
    ]
    for first, _ in small:
        first.start()
    halves = ((0, feats // 2), (feats // 2, feats))
    picks = [
        [
            pltpu.make_async_copy(
                arrived_hbm.at[slot_ref[f]], emb_v.at[:, f * 128 : (f + 1) * 128], sem.at[2 + f]
            )
            for f in range(lo, hi)
        ]
        for lo, hi in halves
    ]
    for half in picks:
        for pick in half:
            pick.start()
    outs = []
    for first, second in small:
        first.wait()
        second.start()
        outs.append(second)
    for n, (lo, hi) in enumerate(halves):
        for pick in picks[n]:
            pick.wait()
        cols = slice(lo * 128, hi * 128)
        outs.append(pltpu.make_async_copy(emb_v.at[:, cols], emb_hbm.at[:, cols], sem.at[2 + feats + n]))
        outs[-1].start()
    for out in outs:
        out.wait()


def on_device(
    next_ids, next_lengths, slot_of_table, tables, cross_input, cotangent, up_weight, down_weight
):
    examples, entries = next_ids.shape
    feats = slot_of_table.shape[0]
    slots, rows_each, embed = tables.shape
    width = cross_input.shape[1]
    rank = up_weight.shape[0]
    per_y = width // X // YL
    per_z = per_y // Z
    anywhere = pl.BlockSpec(memory_space=pl.ANY)
    vmem, dma = pltpu.VMEM, pltpu.SemaphoreType.DMA
    grads = (jax.ShapeDtypeStruct((32, per_z), F32), jax.ShapeDtypeStruct((32, per_z), F32))
    arrived, gup, gdown = pl.pallas_call(
        kernel,
        out_shape=(jax.ShapeDtypeStruct((32, examples, embed), BF16), *grads),
        in_specs=[anywhere] * 8,
        out_specs=(anywhere,) * 3,
        scratch_shapes=[
            vmem((examples, entries), jnp.int32),
            vmem((feats, examples), jnp.int32),
            vmem((1, feats), jnp.int32),
            vmem((8, 16, examples), jnp.int32),
            vmem((8, 16, examples), jnp.int32),
            vmem((8, 4, 8, examples), jnp.int32),
            pltpu.SMEM((2, 8, examples), jnp.int32),
            vmem((slots * rows_each, embed), BF16),
            vmem((slots * rows_each + 8, embed), F32),
            vmem((examples, width), BF16),
            vmem((examples, width), BF16),
            vmem((rank, width), BF16),
            vmem((width, rank), BF16),
            vmem((examples, width), BF16),
            vmem((examples, rank), BF16),
            vmem((examples, rank), BF16),
            vmem((2, width, 128), BF16),
            vmem((2, width, 128), BF16),
            vmem((2, width, 128), F32),
            vmem((2, width, 128), BF16),
            vmem((2, 2, per_y, 128), BF16),
            vmem((2, 2, per_y, 128), BF16),
            vmem((2, 2, per_y, 128), BF16),
            vmem((2, 2, per_y, 128), BF16),
            vmem((2, per_y, 128), F32),
            vmem((2, Z, 80, 128), BF16),
            vmem((2, Z - 1, 80, 128), BF16),
            vmem((2, 80, 128), BF16),
            vmem((Y - 1, 80, 128), BF16),
            vmem((128, 128), F32),
            vmem((32, per_z), F32),
            vmem((32, per_z), F32),
            vmem((2 * examples, embed), F32),
            vmem((8, 4, examples, embed), BF16),
            dma((8,)),
            dma((2,)),
            dma((8,)),
            dma((8,)),
            dma((8,)),
            dma((8,)),
            dma((4,)),
            dma((4,)),
            dma((4,)),
            dma((4,)),
            dma((4,)),
            dma((4,)),
            dma((2 * Z,)),
            dma((2 * Z,)),
            dma((Y,)),
            dma((Y,)),
            dma((8,)),
            dma((8,)),
        ],
        compiler_params=pltpu.CompilerParams(
            collective_id=0, has_side_effects=True, vmem_limit_bytes=60 * 2**20
        ),
    )(
        next_ids,
        next_lengths.T,
        slot_of_table.reshape(1, feats),
        tables.reshape(slots * rows_each, embed),
        cross_input,
        cotangent,
        up_weight,
        down_weight,
    )
    emb, gup, gdown = pl.pallas_call(
        finish,
        out_shape=(jax.ShapeDtypeStruct((examples, feats * embed), BF16), *grads),
        in_specs=[pl.BlockSpec(memory_space=pltpu.SMEM)] + [anywhere] * 3,
        out_specs=(anywhere,) * 3,
        scratch_shapes=[
            vmem((examples, feats * embed), BF16),
            vmem((32, per_z), F32),
            vmem((32, per_z), F32),
            dma((feats + 4,)),
        ],
    )(slot_of_table, arrived, gup, gdown)
    return emb, gup, gdown.T


def solution(mesh):
    return jax.shard_map(
        on_device,
        mesh=mesh,
        in_specs=(
            P(("grp", "tbl"), None),
            P(("grp", "tbl"), None),
            P(),
            P("tbl", None, None),
            P(("grp", "tbl"), None),
            P(("grp", "tbl"), None),
            P(),
            P(),
        ),
        out_specs=(P(("grp", "tbl"), None), P("tbl", "grp"), P("grp", "tbl")),
        check_vma=False,
    )
```
